768 devices in a mesh: samp: 64 (over y, x, core), sx: 6 (over z_lo), sy: 2 (over z_hi).
Axes of the slice: x: 4, y: 8, z: 12 (z_hi: 2, z_lo: 6; z = z_hi * 6 + z_lo), core: 2. Of those that a mesh axis runs over, the one named last changes fastest.
Arguments:
- volume: bfloat16 [64, 32, 12, 16, 128], P('samp', None, 'sx', 'sy'), may hold values from -6 to 6
- kernel: bfloat16 [64, 32, 3, 3, 3], replicated, may hold values from -0.21875 to 0.21875
- bias: float32 [64], replicated, may hold values from -4 to 4
- upstream: bfloat16 [64, 64, 12, 16, 128], P('samp', None, 'sx', 'sy'), may hold values from -6 to 6
Outputs:
- activated: bfloat16 [64, 64, 12, 16, 128], P('samp', None, 'sx', 'sy')
- input_grad: bfloat16 [64, 32, 12, 16, 128], P('samp', None, 'sx', 'sy')
- filter_grad: float32 [64, 32, 3, 3, 3], replicated
- bias_grad: float32 [64], replicated
The draws below stay inside these ranges and needn't reach their ends.
All inputs are finite; a program needn't handle non-finite values.
Results may differ from the reference program's by a relative error of at most 0.0065.
Values may be sent and summed in bfloat16 or wider, within the bound.
No kernel may reach another device: no remote copies, remote signals or barrier semaphores. Data moves between devices by JAX's collectives and lax.ppermute only.
A program may use at most 64 MiB of HBM per device.

```python
import jax
import jax.numpy as jnp
from jax import lax

CIN = 32
COUT = 64
Z = 128
B = 64
X = 12
Y = 16


def levels(stream_key, dims, pieces, least, largest):
    gain = 1.0
    for position, shards_of in pieces:
        steps = jax.random.uniform(jax.random.fold_in(jax.random.fold_in(stream_key, 6), position), (shards_of,), jnp.float32, least / len(pieces), largest / len(pieces))
        gain = gain * jnp.repeat(jnp.exp(steps), dims[position] // shards_of).reshape((-1,) + (1,) * (len(dims) - 1 - position))
    return gain


def noise(own_key, dims, spread, bound, shards=(), kind=jnp.bfloat16):
    values = spread * jax.random.normal(own_key, dims, jnp.float32)
    if shards:
        values = values * levels(own_key, dims, shards, -0.22, 0.18)
    return jnp.clip(values, -bound, bound).astype(kind)


def setup_inputs(seed: int = 0) -> dict:
    keys = jax.random.split(jax.random.key(seed), 5)
    return {
        "volume": noise(keys[0], (B, CIN, X, Y, Z), 1.0, 6.0, ((0, 64), (2, 6), (3, 2))),
        "kernel": noise(keys[1], (COUT, CIN, 3, 3, 3), (27 * CIN) ** -0.5, 0.21875),
        "bias": noise(keys[2], (COUT,), 1.0, 4.0, (), jnp.float32),
        "upstream": noise(keys[3], (B, COUT, X, Y, Z), 1.0, 6.0, ((0, 64), (2, 6), (3, 2))),
    }


def conv_forward(padded, kernel, rows, cols, depth):
    total = None
    for a in range(3):
        for b in range(3):
            for c in range(3):
                piece = padded[:, a:a + rows, b:b + cols, c:c + depth].reshape(padded.shape[0], -1)
                term = jnp.dot(kernel[:, :, a, b, c], piece, preferred_element_type=jnp.float32)
                total = term if total is None else total + term
    return total.reshape(kernel.shape[0], rows, cols, depth)

def conv_backward(padded, kernel, rows, cols, depth):
    total = None
    for a in range(3):
        for b in range(3):
            for c in range(3):
                piece = padded[:, 2 - a:2 - a + rows, 2 - b:2 - b + cols, 2 - c:2 - c + depth].reshape(padded.shape[0], -1)
                term = jnp.dot(kernel[:, :, a, b, c].T, piece, preferred_element_type=jnp.float32)
                total = term if total is None else total + term
    return total.reshape(kernel.shape[1], rows, cols, depth)

def filter_terms(padded, delta, rows, cols, depth):
    flat_delta = delta.reshape(delta.shape[0], -1)
    terms = []
    for a in range(3):
        for b in range(3):
            for c in range(3):
                piece = padded[:, a:a + rows, b:b + cols, c:c + depth].reshape(padded.shape[0], -1)
                terms.append(jnp.dot(flat_delta, piece.T, preferred_element_type=jnp.float32))
    return jnp.stack(terms, axis=-1).reshape(delta.shape[0], padded.shape[0], 3, 3, 3)

def one_sample(items, kernel, bias):
    sample, grad_out = items
    rows, cols, depth = (sample.shape[1], sample.shape[2], sample.shape[3])
    padded = jnp.pad(sample, ((0, 0), (1, 1), (1, 1), (1, 1)))
    pre = conv_forward(padded, kernel, rows, cols, depth) + bias[:, None, None, None]
    activated = (0.3 * pre + 0.7 * jax.nn.softplus(pre)).astype(jnp.bfloat16)
    delta = (grad_out.astype(jnp.float32) * (0.3 + 0.7 * jax.nn.sigmoid(pre))).astype(jnp.bfloat16)
    delta_pad = jnp.pad(delta, ((0, 0), (1, 1), (1, 1), (1, 1)))
    input_grad = conv_backward(delta_pad, kernel, rows, cols, depth).astype(jnp.bfloat16)
    wgrad = filter_terms(padded, delta, rows, cols, depth)
    bgrad = lax.optimization_barrier(jnp.sum(delta.astype(jnp.float32), axis=(1, 2, 3)))
    return (activated, input_grad, wgrad, bgrad)

def reference(volume, kernel, bias, upstream):
    activated, input_grad, wgrad, bgrad = lax.map(lambda items: one_sample(items, kernel, bias), (volume, upstream))
    norm = 1.0 / jnp.sqrt(jnp.float32(volume.shape[0] * volume.shape[2] * volume.shape[3] * volume.shape[4]))
    return (activated, input_grad, lax.optimization_barrier(jnp.sum(wgrad, axis=0)) * norm, lax.optimization_barrier(jnp.sum(bgrad, axis=0)) * norm)
```

```python
import jax
import jax.numpy as jnp
from jax import lax
from jax.experimental import pallas as pl
from jax.experimental.pallas import tpu as pltpu
from jax.sharding import PartitionSpec as P

BF = jnp.bfloat16
F32 = jnp.float32
CI, CO, NX, NY, NZ = 32, 64, 2, 8, 128
GROUP = ("sx", "sy")
NT_DIMS = (((1,), (1,)), ((), ()))
VM = pl.BlockSpec(memory_space=pltpu.VMEM)
SM = pl.BlockSpec(memory_space=pltpu.SMEM)
ROWS = 480


def call(body, outs, scratch=(), n_in=1, smem=0, flops=0):
    return pl.pallas_call(
        body,
        out_shape=outs,
        in_specs=[SM] * smem + [VM] * (n_in - smem),
        out_specs=jax.tree.map(lambda _: VM, outs),
        scratch_shapes=list(scratch),
        cost_estimate=pl.CostEstimate(flops=flops, bytes_accessed=1 << 20, transcendentals=0),
    )


def turn_volume(sy_ref, v_ref, t_ref, edge_ref, buf):
    buf[...] = v_ref[...].astype(F32).reshape(CI * NX * NY, NZ)
    for x in range(NX):
        for y in range(NY):
            t_ref[x, y] = buf[pl.ds(x * NY + y, CI, stride=NX * NY), :].astype(BF)
    edge = (1 - sy_ref[0]) * (NY - 1)
    for x in range(NX):
        edge_ref[x] = buf[pl.ds(x * NY + edge, CI, stride=NX * NY), :].astype(BF)


def prepare(w_ref, u_ref, fwd_ref, bwd_ref, t_ref, buf):
    eye = (
        lax.broadcasted_iota(jnp.int32, (CO, CO), 0) == lax.broadcasted_iota(jnp.int32, (CO, CO), 1)
    ).astype(BF)
    for c in range(3):
        taps = jnp.concatenate(
            [w_ref[(ab * 3 + c) * CI : (ab * 3 + c + 1) * CI, :] for ab in range(9)], axis=0
        )
        fwd_ref[c * CO : (c + 1) * CO, :] = lax.dot_general(
            eye, taps, NT_DIMS, preferred_element_type=F32
        ).astype(BF)
        for ab in range(9):
            back = (2 - ab // 3) * 3 + 2 - ab % 3
            bwd_ref[c * CI : (c + 1) * CI, back * CO : (back + 1) * CO] = w_ref[
                (ab * 3 + c) * CI : (ab * 3 + c + 1) * CI, :
            ]
    buf[...] = u_ref[...].astype(F32).reshape(CO * NX * NY, NZ)
    for p in range(NX * NY):
        t_ref[p] = buf[pl.ds(p, CO, stride=NX * NY), :].astype(BF)


def fill(ext, sy, own, before, after, row, corner_lo, corner_hi):
    for x in range(NX):
        for y in range(NY):
            ext[x + 1, y + 1] = own[x, y]
    for y in range(NY):
        ext[0, y + 1] = before[y]
        ext[3, y + 1] = after[y]
    far = (1 - sy) * (NY + 1)
    near = sy * (NY + 1)
    nothing = jnp.zeros(ext.shape[2:], BF)
    for x in range(4):
        ext[x, near] = nothing
    ext[0, far] = corner_lo
    ext[1, far] = row[0]
    ext[2, far] = row[1]
    ext[3, far] = corner_hi


def window(ext, x, y, channels):
    parts = []
    for dy in range(2):
        parts.append(
            jnp.concatenate(
                [ext[x + a, y + dy : y + dy + 3].reshape(3 * channels, NZ) for a in range(3)], axis=0
            )
        )
    return parts


def moved(v, shift):
    lane = lax.broadcasted_iota(jnp.int32, v.shape, 1)
    if shift == 1:
        return jnp.where(lane == 0, 0.0, pltpu.roll(v, 1, 1))
    return jnp.where(lane == NZ - 1, 0.0, pltpu.roll(v, NZ - 1, 1))


def forward(
    sy_ref, t_ref, before_ref, after_ref, row_ref, lo_ref, hi_ref, fwd_ref, up_ref, bias_ref,
    act_ref, delta_ref, edge_ref, sum_ref, ext, acc,
):
    sy = sy_ref[0]
    fill(ext, sy, t_ref, before_ref, after_ref, row_ref, lo_ref[...], hi_ref[...])
    acc[...] = jnp.zeros_like(acc)
    ones = jnp.ones((16, 2 * NZ), BF)
    none = jnp.zeros((CO, 2 * NZ), BF)
    for x in range(NX):
        for y in range(0, NY, 2):
            first, second = window(ext, x, y, CI)
            cols = jnp.concatenate([first, second], axis=1)
            part = jnp.dot(fwd_ref[...], cols, preferred_element_type=F32)
            shifted = [[], [], []]
            for k in range(2):
                at = slice(k * NZ, (k + 1) * NZ)
                pre = (
                    moved(part[:CO, at], 1)
                    + part[CO : 2 * CO, at]
                    + moved(part[2 * CO :, at], -1)
                    + bias_ref[...]
                )
                e = jnp.exp(-jnp.abs(pre))
                r = 1.0 / (1.0 + e)
                sig = jnp.where(pre >= 0, r, e * r)
                soft = jnp.maximum(pre, 0.0) + jnp.log1p(e)
                p = x * NY + y + k
                act_ref[p] = (0.3 * pre + 0.7 * soft).astype(BF)
                d = (up_ref[p].astype(F32) * (0.3 + 0.7 * sig)).astype(BF)
                delta_ref[x, y + k] = d
                wide = d.astype(F32)
                shifted[0].append(moved(wide, -1).astype(BF))
                shifted[1].append(d)
                shifted[2].append(moved(wide, 1).astype(BF))
            right = jnp.concatenate(
                [jnp.concatenate(s, axis=1) for s in shifted] + [none], axis=0
            )
            left = jnp.concatenate([cols, ones], axis=0)
            acc[...] += lax.dot_general(left, right, NT_DIMS, preferred_element_type=F32)
    edge = (1 - sy) * (NY - 1)
    for x in range(NX):
        edge_ref[x] = delta_ref[x, edge]
    n = 9 * CI
    sum_ref[0:n, :] = acc[0:n, 0:NZ].astype(sum_ref.dtype)
    half = n // 2
    sum_ref[n : n + half, :] = (
        acc[0:half, NZ:] + pltpu.roll(acc[half:n, NZ:], CO, 1)
    ).astype(sum_ref.dtype)
    sum_ref[n + half : n + half + 8, :] = acc[n : n + 8, 0:NZ].astype(sum_ref.dtype)
    sum_ref[n + half + 8 :, :] = jnp.zeros((ROWS - n - half - 8, NZ), sum_ref.dtype)


def backward(
    sy_ref, d_ref, before_ref, after_ref, row_ref, lo_ref, hi_ref, bwd_ref, act_ref,
    out_ref, grad_ref, ext, wide, narrow,
):
    for p in range(NX * NY):
        wide[pl.ds(p, CO, stride=NX * NY), :] = act_ref[p].astype(F32)
    out_ref[...] = wide[...].reshape(CO, NX, NY, NZ).astype(BF)
    fill(ext, sy_ref[0], d_ref, before_ref, after_ref, row_ref, lo_ref[...], hi_ref[...])
    for x in range(NX):
        for y in range(0, NY, 2):
            first, second = window(ext, x, y, CO)
            cols = jnp.concatenate([first, second], axis=1)
            part = jnp.dot(bwd_ref[...], cols, preferred_element_type=F32)
            for k in range(2):
                at = slice(k * NZ, (k + 1) * NZ)
                g = (
                    moved(part[:CI, at], -1)
                    + part[CI : 2 * CI, at]
                    + moved(part[2 * CI :, at], 1)
                )
                narrow[pl.ds(x * NY + y + k, CI, stride=NX * NY), :] = g
    grad_ref[...] = narrow[...].reshape(CI, NX, NY, NZ).astype(BF)


def finish(norm_ref, s_ref, w_ref, b_ref):
    norm = norm_ref[0]
    n, half = 9 * CI, 9 * CI // 2
    total = s_ref[...].astype(F32) * norm
    for ab in range(9):
        at = ab * CI
        w_ref[(ab * 3) * CI : (ab * 3 + 1) * CI, :] = total[at : at + CI, :CO]
        w_ref[(ab * 3 + 1) * CI : (ab * 3 + 2) * CI, :] = pltpu.roll(
            total[at : at + CI, :], CO, 1
        )[:, :CO]
    last = jnp.concatenate(
        [total[n : n + half], pltpu.roll(total[n : n + half], CO, 1)], axis=0
    )[:, :CO]
    for ab in range(9):
        w_ref[(ab * 3 + 2) * CI : (ab * 3 + 3) * CI, :] = last[ab * CI : (ab + 1) * CI]
    b_ref[...] = pltpu.roll(total[n + half : n + half + 8, :], CO, 1)[:, :CO]


def everywhere(blocks, axis):
    return lax.all_to_all(blocks, axis, 0, 0, tiled=True)


def copies(share, axis):
    return everywhere(jnp.broadcast_to(share[None], (lax.axis_size(axis), *share.shape)), axis)


def reduced(part):
    groups = lax.axis_size(GROUP)
    send = part.reshape(groups, ROWS // groups, NZ)
    share = jnp.sum(everywhere(send, GROUP).astype(F32), axis=0).astype(part.dtype)
    share = jnp.sum(copies(share, "samp").astype(F32), axis=0).astype(part.dtype)
    return copies(share, GROUP).reshape(ROWS, NZ)


def neighbours(t, row):
    n = lax.axis_size("sx")
    up = [(i, i + 1) for i in range(n - 1)]
    down = [(j, i) for i, j in up]
    before = lax.ppermute(t[NX - 1], "sx", up)
    after = lax.ppermute(t[0], "sx", down)
    here = (1 - lax.axis_index("sy")) * (NY - 1)
    lo = lax.dynamic_index_in_dim(before, here, 0, keepdims=True)
    hi = lax.dynamic_index_in_dim(after, here, 0, keepdims=True)
    swapped = lax.ppermute(jnp.concatenate([lo, row, hi], axis=0), "sy", [(0, 1), (1, 0)])
    return before, after, swapped[1:3], swapped[0], swapped[3]


def per_device(volume, kernel, bias, upstream, dt=BF):
    s = jax.ShapeDtypeStruct
    sy = lax.axis_index("sy").astype(jnp.int32).reshape(1)
    taps = jnp.transpose(kernel, (2, 3, 4, 1, 0)).reshape(27 * CI, CO)
    t, row = call(
        turn_volume,
        (s((NX, NY, CI, NZ), BF), s((NX, CI, NZ), BF)),
        [pltpu.VMEM((CI * NX * NY, NZ), F32)], 2, 1, 10**8,
    )(sy, volume[0])
    fwd, bwd, up = call(
        prepare,
        (s((3 * CO, 9 * CI), BF), s((3 * CI, 9 * CO), BF), s((NX * NY, CO, NZ), BF)),
        [pltpu.VMEM((CO * NX * NY, NZ), F32)], 2, 0, 10**9,
    )(taps, upstream[0])
    bias_wide = jnp.broadcast_to(bias[:, None], (CO, NZ))
    act, delta, edge, part = call(
        forward,
        (s((NX * NY, CO, NZ), BF), s((NX, NY, CO, NZ), BF), s((NX, CO, NZ), BF), s((ROWS, NZ), dt)),
        [pltpu.VMEM((4, NY + 2, CI, NZ), BF), pltpu.VMEM((9 * CI + 16, 2 * NZ), F32)], 10, 1, 4 * 10**9,
    )(sy, t, *neighbours(t, row), fwd, up, bias_wide)
    summed = reduced(part)
    out, grad = call(
        backward,
        (s((CO, NX, NY, NZ), BF), s((CI, NX, NY, NZ), BF)),
        [
            pltpu.VMEM((4, NY + 2, CO, NZ), BF),
            pltpu.VMEM((CO * NX * NY, NZ), F32),
            pltpu.VMEM((CI * NX * NY, NZ), F32),
        ],
        9, 1, 4 * 10**9,
    )(sy, delta, *neighbours(delta, edge), bwd, act)
    whole = lax.axis_size("samp") * lax.axis_size(GROUP) * NX * NY * NZ
    norm = (1.0 / jnp.sqrt(jnp.float32(whole))).reshape(1)
    w, b = call(finish, (s((27 * CI, CO), F32), s((8, CO), F32)), (), 2, 1, 10**8)(norm, summed)
    wgrad = jnp.transpose(w.reshape(3, 3, 3, CI, CO), (4, 3, 0, 1, 2))
    return out[None], grad[None], wgrad, b[0]


def solution(mesh):
    spec = P("samp", None, "sx", "sy", None)
    return jax.shard_map(
        per_device, mesh=mesh, in_specs=(spec, P(), P(), spec), out_specs=(spec, spec, P(), P()), check_vma=False
    )
```

```python
import jax
import jax.numpy as jnp
from jax import lax
from jax.experimental import pallas as pl
from jax.experimental.pallas import tpu as pltpu
from jax.sharding import Mesh
from jax.sharding import PartitionSpec as P


BF = jnp.bfloat16
F32 = jnp.float32
CI, CO, NX, NY, NZ = 32, 64, 2, 8, 128
GROUP = ("core", "sx", "sy")
SAMP = ("plane", "core")
NT_DIMS = (((1,), (1,)), ((), ()))
VM = pl.BlockSpec(memory_space=pltpu.VMEM)
SM = pl.BlockSpec(memory_space=pltpu.SMEM)
ROWS = 512


def call(body, outs, scratch=(), n_in=1, smem=0, flops=0):
    inner = pl.pallas_call(
        body,
        out_shape=outs,
        in_specs=[SM] * smem + [VM] * (n_in - smem),
        out_specs=jax.tree.map(lambda _: VM, outs),
        scratch_shapes=list(scratch),
        cost_estimate=pl.CostEstimate(flops=flops, bytes_accessed=1 << 20, transcendentals=0),
    )

    def run(*args):
        near = [pltpu.with_memory_space_constraint(a, pltpu.VMEM) for a in args[smem:]]
        return inner(*args[:smem], *near)

    return run


def turn_volume(sy_ref, v_ref, lo_ref, hi_ref, edge_ref, buf):
    buf[...] = v_ref[...].astype(F32).reshape(CI * NX * NY, NZ)
    for x, t_ref in enumerate((lo_ref, hi_ref)):
        for y in range(NY):
            t_ref[y] = buf[pl.ds(x * NY + y, CI, stride=NX * NY), :].astype(BF)
    edge = (1 - sy_ref[0]) * (NY - 1)
    for x in range(NX):
        edge_ref[x] = buf[pl.ds(x * NY + edge, CI, stride=NX * NY), :].astype(BF)


def prepare(w_ref, b_ref, u_ref, fwd_ref, bwd_ref, t_ref, wide_ref, buf):
    eye = lax.broadcasted_iota(jnp.int32, (CO, CO), 0) == lax.broadcasted_iota(jnp.int32, (CO, CO), 1)
    column = jnp.sum(jnp.where(eye, b_ref[...], 0.0), axis=1, keepdims=True)
    wide_ref[...] = jnp.broadcast_to(column, (CO, NZ))
    eye = eye.astype(BF)
    for c in range(3):
        taps = jnp.concatenate(
            [w_ref[(ab * 3 + c) * CI : (ab * 3 + c + 1) * CI, :] for ab in range(9)], axis=0
        )
        fwd_ref[c * CO : (c + 1) * CO, :] = lax.dot_general(
            eye, taps, NT_DIMS, preferred_element_type=F32
        ).astype(BF)
        for ab in range(9):
            back = (2 - ab // 3) * 3 + 2 - ab % 3
            bwd_ref[c * CI : (c + 1) * CI, back * CO : (back + 1) * CO] = w_ref[
                (ab * 3 + c) * CI : (ab * 3 + c + 1) * CI, :
            ]
    buf[...] = u_ref[...].astype(F32).reshape(CO * NX * NY, NZ)
    for p in range(NX * NY):
        t_ref[p] = buf[pl.ds(p, CO, stride=NX * NY), :].astype(BF)


def fill(ext, sy, planes, rows):
    for x, plane in enumerate(planes):
        for y in range(NY):
            ext[x, y + 1] = plane[y]
    far = (1 - sy) * (NY + 1)
    near = sy * (NY + 1)
    nothing = jnp.zeros(ext.shape[2:], BF)
    for x in range(4):
        ext[x, near] = nothing
        ext[x, far] = rows[x]


def window(ext, x, y, channels):
    parts = []
    for dy in range(2):
        parts.append(
            jnp.concatenate(
                [ext[x + a, pl.ds(y + dy, 3)].reshape(3 * channels, NZ) for a in range(3)], axis=0
            )
        )
    return parts


def moved(v, shift):
    lane = lax.broadcasted_iota(jnp.int32, v.shape, 1)
    if shift == 1:
        return jnp.where(lane == 0, 0.0, pltpu.roll(v, 1, 1))
    return jnp.where(lane == NZ - 1, 0.0, pltpu.roll(v, NZ - 1, 1))


def two_rows(ext, x, y, at_y, fwd_ref, up_ref, bias_ref, act_ref, delta_refs):
    ones = jnp.ones((16, 2 * NZ), BF)
    none = jnp.zeros((CO, 2 * NZ), BF)
    first, second = window(ext, x, y, CI)
    cols = jnp.concatenate([first, second], axis=1)
    part = jnp.dot(fwd_ref[...], cols, preferred_element_type=F32)
    shifted = [[], [], []]
    for k in range(2):
        at = slice(k * NZ, (k + 1) * NZ)
        pre = (
            moved(part[:CO, at], 1)
            + part[CO : 2 * CO, at]
            + moved(part[2 * CO :, at], -1)
            + bias_ref[...]
        )
        e = jnp.exp(-jnp.abs(pre))
        r = 1.0 / (1.0 + e)
        sig = jnp.where(pre >= 0, r, e * r)
        soft = jnp.maximum(pre, 0.0) + jnp.log1p(e)
        p = x * NY + at_y + k
        act_ref[p] = (0.3 * pre + 0.7 * soft).astype(BF)
        d = (up_ref[p].astype(F32) * (0.3 + 0.7 * sig)).astype(BF)
        delta_refs[x][at_y + k] = d
        wide = d.astype(F32)
        shifted[0].append(moved(wide, -1).astype(BF))
        shifted[1].append(d)
        shifted[2].append(moved(wide, 1).astype(BF))
    right = jnp.concatenate([jnp.concatenate(s, axis=1) for s in shifted] + [none], axis=0)
    left = jnp.concatenate([cols, ones], axis=0)
    return lax.dot_general(left, right, NT_DIMS, preferred_element_type=F32)


def forward_near(
    sy_ref, before_ref, lo_ref, hi_ref, after_ref, fwd_ref, up_ref, bias_ref,
    act_ref, dlo_ref, dhi_ref, acc, ext,
):
    sy = sy_ref[0]
    for x, plane in enumerate((before_ref, lo_ref, hi_ref, after_ref)):
        for y in range(NY):
            ext[x, y + 1] = plane[y]
        ext[x, sy * (NY + 1)] = jnp.zeros(ext.shape[2:], BF)
        ext[x, (1 - sy) * (NY + 1)] = jnp.zeros(ext.shape[2:], BF)
    for x in range(NX):
        for j in range(NY // 2 - 1):
            y = 2 * j + 2 * sy
            part = two_rows(ext, x, y, y, fwd_ref, up_ref, bias_ref, act_ref, (dlo_ref, dhi_ref))
            if x + j:
                acc[...] += part
            else:
                acc[...] = part
        far = (1 - sy) * (NY - 2)
        for k in range(2):
            act_ref[x * NY + far + k] = jnp.zeros((CO, NZ), BF)
            (dlo_ref, dhi_ref)[x][far + k] = jnp.zeros((CO, NZ), BF)


def forward_far(
    sy_ref, before_ref, lo_ref, hi_ref, after_ref, row_ref, fwd_ref, up_ref, bias_ref,
    act_in, dlo_in, dhi_in, acc_in, act_ref, dlo_ref, dhi_ref, edge_ref, sum_ref, ext, acc,
):
    sy = sy_ref[0]
    act_ref[...] = act_in[...]
    dlo_ref[...] = dlo_in[...]
    dhi_ref[...] = dhi_in[...]
    rows = row_ref
    for x, plane in enumerate((before_ref, lo_ref, hi_ref, after_ref)):
        for y in range(3):
            ext[x, sy + y] = plane[(1 - sy) * (NY - 3) + y]
        ext[x, 3 * (1 - sy)] = rows[x]
    far = (1 - sy) * (NY - 2)
    acc[...] = acc_in[...]
    for x in range(NX):
        acc[...] += two_rows(ext, x, 0, far, fwd_ref, up_ref, bias_ref, act_ref, (dlo_ref, dhi_ref))
    edge = (1 - sy) * (NY - 1)
    edge_ref[0] = dlo_ref[edge]
    edge_ref[1] = dhi_ref[edge]
    n = 9 * CI
    sum_ref[0:n, :] = acc[0:n, 0:NZ].astype(sum_ref.dtype)
    half = n // 2
    sum_ref[n : n + half, :] = (
        acc[0:half, NZ:] + pltpu.roll(acc[half:n, NZ:], CO, 1)
    ).astype(sum_ref.dtype)
    sum_ref[n + half : n + half + 8, :] = acc[n : n + 8, 0:NZ].astype(sum_ref.dtype)
    sum_ref[n + half + 8 :, :] = jnp.zeros((ROWS - n - half - 8, NZ), sum_ref.dtype)


def backward(
    sy_ref, before_ref, lo_ref, hi_ref, after_ref, row_ref, bwd_ref, act_ref,
    out_ref, grad_ref, ext, wide, narrow,
):
    for p in range(NX * NY):
        wide[pl.ds(p, CO, stride=NX * NY), :] = act_ref[p].astype(F32)
    out_ref[...] = wide[...].reshape(CO, NX, NY, NZ).astype(BF)
    fill(ext, sy_ref[0], (before_ref, lo_ref, hi_ref, after_ref), row_ref)
    for x in range(NX):
        for y in range(0, NY, 2):
            first, second = window(ext, x, y, CO)
            cols = jnp.concatenate([first, second], axis=1)
            part = jnp.dot(bwd_ref[...], cols, preferred_element_type=F32)
            for k in range(2):
                at = slice(k * NZ, (k + 1) * NZ)
                g = (
                    moved(part[:CI, at], -1)
                    + part[CI : 2 * CI, at]
                    + moved(part[2 * CI :, at], 1)
                )
                narrow[pl.ds(x * NY + y + k, CI, stride=NX * NY), :] = g
    grad_ref[...] = narrow[...].reshape(CI, NX, NY, NZ).astype(BF)


def finish(norm_ref, s_ref, w_ref, b_ref):
    norm = norm_ref[0]
    n, half = 9 * CI, 9 * CI // 2
    total = s_ref[...].astype(F32) * norm
    for ab in range(9):
        at = ab * CI
        w_ref[(ab * 3) * CI : (ab * 3 + 1) * CI, :] = total[at : at + CI, :CO]
        w_ref[(ab * 3 + 1) * CI : (ab * 3 + 2) * CI, :] = pltpu.roll(
            total[at : at + CI, :], CO, 1
        )[:, :CO]
    last = jnp.concatenate(
        [total[n : n + half], pltpu.roll(total[n : n + half], CO, 1)], axis=0
    )[:, :CO]
    for ab in range(9):
        w_ref[(ab * 3 + 2) * CI : (ab * 3 + 3) * CI, :] = last[ab * CI : (ab + 1) * CI]
    b_ref[...] = pltpu.roll(total[n + half : n + half + 8, :], CO, 1)[0:1, :CO]


def everywhere(blocks, axis):
    return lax.all_to_all(blocks, axis, 0, 0, tiled=True)


def copies(share, axis):
    return everywhere(jnp.broadcast_to(share[None], (lax.axis_size(axis), *share.shape)), axis)


def total(blocks):
    return jnp.sum(blocks.astype(F32), axis=0).astype(blocks.dtype)


def reduced(part):
    shares = lax.axis_size("plane")
    share = everywhere(part.reshape(shares, ROWS // shares, NZ), "plane")
    share = total(share)
    share = copies(share, GROUP)
    share = total(share)
    share = copies(share, "plane")
    return share.reshape(ROWS, NZ)


def neighbours(first, last, row):
    n = lax.axis_size("sx")
    up = [(i, i + 1) for i in range(n - 1)]
    down = [(j, i) for i, j in up]
    before = lax.ppermute(last, "sx", up)
    after = lax.ppermute(first, "sx", down)
    here = (1 - lax.axis_index("sy")) * (NY - 1)
    lo = lax.dynamic_index_in_dim(before, here, 0, keepdims=True)
    hi = lax.dynamic_index_in_dim(after, here, 0, keepdims=True)
    swapped = lax.ppermute(jnp.concatenate([lo, row, hi], axis=0), "sy", [(0, 1), (1, 0)])
    return before, first, last, after, swapped


def per_device(volume, kernel, bias, upstream, dt=BF):
    s = pltpu.VMEM
    sy = lax.axis_index("sy").astype(jnp.int32).reshape(1)
    taps = jnp.transpose(kernel, (2, 3, 4, 1, 0)).reshape(27 * CI, CO)
    first, last, row = call(
        turn_volume,
        (s((NY, CI, NZ), BF), s((NY, CI, NZ), BF), s((NX, CI, NZ), BF)),
        [pltpu.VMEM((CI * NX * NY, NZ), F32)], 2, 1, 10**8,
    )(sy, volume[0])
    fwd, bwd, up, bias_wide = call(
        prepare,
        (s((3 * CO, 9 * CI), BF), s((3 * CI, 9 * CO), BF), s((NX * NY, CO, NZ), BF), s((CO, NZ), F32)),
        [pltpu.VMEM((CO * NX * NY, NZ), F32)], 3, 0, 10**9,
    )(taps, bias.reshape(1, CO), upstream[0])
    around = list(neighbours(first, last, row))
    shapes = (s((NX * NY, CO, NZ), BF), s((NY, CO, NZ), BF), s((NY, CO, NZ), BF))
    sums = (9 * CI + 16, 2 * NZ)
    early = call(
        forward_near, (*shapes, s(sums, F32)),
        [pltpu.VMEM((4, NY + 2, CI, NZ), BF)], 8, 1, 3 * 10**9,
    )(sy, *around[:4], fwd, up, bias_wide)
    act, dfirst, dlast, edge, part = call(
        forward_far, (*shapes, s((NX, CO, NZ), BF), s((ROWS, NZ), dt)),
        [pltpu.VMEM((4, 4, CI, NZ), BF), pltpu.VMEM(sums, F32)], 13, 1, 10**9,
    )(sy, *around, fwd, up, bias_wide, *early)
    summed = reduced(part)
    o = jax.ShapeDtypeStruct
    out, grad = call(
        backward,
        (o((CO, NX, NY, NZ), BF), o((CI, NX, NY, NZ), BF)),
        [
            pltpu.VMEM((4, NY + 2, CO, NZ), BF),
            pltpu.VMEM((CO * NX * NY, NZ), F32),
            pltpu.VMEM((CI * NX * NY, NZ), F32),
        ],
        8, 1, 4 * 10**9,
    )(sy, *neighbours(dfirst, dlast, edge), bwd, act)
    whole = lax.axis_size("plane") * lax.axis_size(GROUP) * NX * NY * NZ
    norm = (1.0 / jnp.sqrt(jnp.float32(whole))).reshape(1)
    w, b = call(finish, (o((27 * CI, CO), F32), o((1, CO), F32)), (), 2, 1, 10**8)(norm, summed)
    wgrad = jnp.transpose(w.reshape(3, 3, 3, CI, CO), (4, 3, 0, 1, 2))
    return out[None], grad[None], wgrad, b.reshape(CO)


def solution(mesh):
    cores = 2
    samp, sx, sy = mesh.devices.shape
    mesh = Mesh(mesh.devices.reshape(samp // cores, cores, sx, sy), ("plane", "core", "sx", "sy"))
    spec = P(SAMP, None, "sx", "sy", None)
    return jax.shard_map(
        per_device, mesh=mesh, in_specs=(spec, P(), P(), spec), out_specs=(spec, spec, P(), P()), check_vma=False
    )
```

```python
import jax
import jax.numpy as jnp
from jax import lax
from jax.experimental import pallas as pl
from jax.experimental.pallas import tpu as pltpu
from jax.sharding import Mesh
from jax.sharding import PartitionSpec as P


BF = jnp.bfloat16
F32 = jnp.float32
CI, CO, NX, NY, NZ = 32, 64, 2, 8, 128
GROUP = ("core", "sx", "sy")
SAMP = ("plane", "core")
NT_DIMS = (((1,), (1,)), ((), ()))
VM = pl.BlockSpec(memory_space=pltpu.VMEM)
SM = pl.BlockSpec(memory_space=pltpu.SMEM)
ROWS = 512


def call(body, outs, scratch=(), n_in=1, smem=0, flops=0):
    inner = pl.pallas_call(
        body,
        out_shape=outs,
        in_specs=[SM] * smem + [VM] * (n_in - smem),
        out_specs=jax.tree.map(lambda _: VM, outs),
        scratch_shapes=list(scratch),
        cost_estimate=pl.CostEstimate(flops=flops, bytes_accessed=1 << 20, transcendentals=0),
    )

    def run(*args):
        near = [pltpu.with_memory_space_constraint(a, pltpu.VMEM) for a in args[smem:]]
        return inner(*args[:smem], *near)

    return run


def turn_volume(sy_ref, v_ref, own_ref, edge_ref, buf):
    buf[...] = v_ref[...].astype(F32).reshape(CI * NX * NY, NZ)
    for x in range(NX):
        for y in range(NY):
            own_ref[x, y] = buf[pl.ds(x * NY + y, CI, stride=NX * NY), :].astype(BF)
    edge = (1 - sy_ref[0]) * (NY - 1)
    for x in range(NX):
        edge_ref[x] = own_ref[x, edge]


def prepare(w_ref, b_ref, u_ref, fwd_ref, bwd_ref, lo_ref, hi_ref, wide_ref, buf):
    eye = lax.broadcasted_iota(jnp.int32, (CO, CO), 0) == lax.broadcasted_iota(jnp.int32, (CO, CO), 1)
    column = jnp.sum(jnp.where(eye, b_ref[...], 0.0), axis=1, keepdims=True)
    wide_ref[...] = jnp.broadcast_to(column, (CO, NZ))
    eye = eye.astype(BF)
    for c in range(3):
        taps = jnp.concatenate(
            [w_ref[(ab * 3 + c) * CI : (ab * 3 + c + 1) * CI, :] for ab in range(9)], axis=0
        )
        fwd_ref[c * CO : (c + 1) * CO, :] = lax.dot_general(
            eye, taps, NT_DIMS, preferred_element_type=F32
        ).astype(BF)
        for ab in range(9):
            back = (2 - ab // 3) * 3 + 2 - ab % 3
            bwd_ref[c * CI : (c + 1) * CI, back * CO : (back + 1) * CO] = w_ref[
                (ab * 3 + c) * CI : (ab * 3 + c + 1) * CI, :
            ]
    buf[...] = u_ref[...].astype(F32).reshape(CO * NX * NY, NZ)
    for y in range(NY):
        lo_ref[y] = buf[pl.ds(y, CO, stride=NX * NY), :].astype(BF)
        hi_ref[y] = buf[pl.ds(NY + y, CO, stride=NX * NY), :].astype(BF)


def window(ext, x, y, channels):
    parts = []
    for dy in range(2):
        parts.append(
            jnp.concatenate(
                [ext[x + a, pl.ds(y + dy, 3)].reshape(3 * channels, NZ) for a in range(3)], axis=0
            )
        )
    return parts


def moved(v, shift):
    lane = lax.broadcasted_iota(jnp.int32, v.shape, 1)
    if shift == 1:
        return jnp.where(lane == 0, 0.0, pltpu.roll(v, 1, 1))
    return jnp.where(lane == NZ - 1, 0.0, pltpu.roll(v, NZ - 1, 1))


def two_rows(ext, x, y, at_y, first_x, fwd_ref, ups, bias_ref, acts, deltas):
    ones = jnp.ones((16, 2 * NZ), BF)
    none = jnp.zeros((CO, 2 * NZ), BF)
    first, second = window(ext, x, y, CI)
    cols = jnp.concatenate([first, second], axis=1)
    part = jnp.dot(fwd_ref[...], cols, preferred_element_type=F32)
    shifted = [[], [], []]
    for k in range(2):
        at = slice(k * NZ, (k + 1) * NZ)
        pre = (
            moved(part[:CO, at], 1)
            + part[CO : 2 * CO, at]
            + moved(part[2 * CO :, at], -1)
            + bias_ref[...]
        )
        e = jnp.exp(-jnp.abs(pre))
        r = 1.0 / (1.0 + e)
        sig = jnp.where(pre >= 0, r, e * r)
        soft = jnp.maximum(pre, 0.0) + jnp.log1p(e)
        act = 0.3 * pre + 0.7 * soft
        grad = ups[x][at_y + k].astype(F32) * (0.3 + 0.7 * sig)
        if x == 0:
            act = jnp.where(first_x, act, 0.0)
            grad = jnp.where(first_x, grad, 0.0)
        acts[x][at_y + k] = act.astype(BF)
        d = grad.astype(BF)
        deltas[x][at_y + k] = d
        wide = d.astype(F32)
        shifted[0].append(moved(wide, -1).astype(BF))
        shifted[1].append(d)
        shifted[2].append(moved(wide, 1).astype(BF))
    right = jnp.concatenate([jnp.concatenate(s, axis=1) for s in shifted] + [none], axis=0)
    left = jnp.concatenate([cols, ones], axis=0)
    return lax.dot_general(left, right, NT_DIMS, preferred_element_type=F32)


def places(send_ref, keep_ref):
    acts = (keep_ref.at[1], keep_ref.at[2], send_ref.at[2])
    return acts, (keep_ref.at[0], send_ref.at[0], send_ref.at[1])


def forward_near(
    sy_ref, sx_ref, own_ref, next_ref, fwd_ref, lo_ref, hi_ref, up_ref, bias_ref,
    send_ref, keep_ref, acc, ext,
):
    sy = sy_ref[0]
    ext[0] = jnp.zeros(ext.shape[1:], BF)
    for x, plane in enumerate((own_ref.at[0], own_ref.at[1], next_ref.at[0], next_ref.at[1])):
        for y in range(NY):
            ext[x + 1, y + 1] = plane[y]
        ext[x + 1, sy * (NY + 1)] = jnp.zeros(ext.shape[2:], BF)
        ext[x + 1, (1 - sy) * (NY + 1)] = jnp.zeros(ext.shape[2:], BF)
    acts, deltas = places(send_ref, keep_ref)
    ups = (lo_ref, hi_ref, up_ref)
    far = (1 - sy) * (NY - 2)
    for x in range(NX + 1):
        for j in range(NY // 2 - 1):
            y = 2 * j + 2 * sy
            part = two_rows(ext, x, y, y, sx_ref[0] == 0, fwd_ref, ups, bias_ref, acts, deltas)
            if x + j:
                acc[...] += part
            else:
                acc[...] = part
        for k in range(2):
            acts[x][far + k] = jnp.zeros((CO, NZ), BF)
            deltas[x][far + k] = jnp.zeros((CO, NZ), BF)


def forward_far(
    sy_ref, sx_ref, own_ref, next_ref, row_ref, fwd_ref, lo_ref, hi_ref, up_ref, bias_ref, send_in, keep_in, acc_in,
    send_ref, keep_ref, edge_ref, sum_ref, ext, acc,
):
    sy = sy_ref[0]
    send_ref[...] = send_in[...]
    keep_ref[...] = keep_in[...]
    ext[0] = jnp.zeros(ext.shape[1:], BF)
    for x, plane in enumerate((own_ref.at[0], own_ref.at[1], next_ref.at[0], next_ref.at[1])):
        for y in range(3):
            ext[x + 1, sy + y] = plane[(1 - sy) * (NY - 3) + y]
        ext[x + 1, 3 * (1 - sy)] = row_ref[x]
    acts, deltas = places(send_ref, keep_ref)
    ups = (lo_ref, hi_ref, up_ref)
    far = (1 - sy) * (NY - 2)
    acc[...] = acc_in[...]
    for x in range(NX + 1):
        acc[...] += two_rows(ext, x, 0, far, sx_ref[0] == 0, fwd_ref, ups, bias_ref, acts, deltas)
    edge = (1 - sy) * (NY - 1)
    edge_ref[0] = jnp.zeros((CO, NZ), BF)
    for x in range(NX + 1):
        edge_ref[x + 1] = deltas[x][edge]
    n = 9 * CI
    sum_ref[0:n, :] = acc[0:n, 0:NZ].astype(sum_ref.dtype)
    half = n // 2
    sum_ref[n : n + half, :] = (
        acc[0:half, NZ:] + pltpu.roll(acc[half:n, NZ:], CO, 1)
    ).astype(sum_ref.dtype)
    sum_ref[n + half : n + half + 8, :] = acc[n : n + 8, 0:NZ].astype(sum_ref.dtype)
    sum_ref[n + half + 8 :, :] = jnp.zeros((ROWS - n - half - 8, NZ), sum_ref.dtype)


def plus(a, b):
    return (a.astype(F32) + b.astype(F32)).astype(BF)


def backward(
    sy_ref, got_ref, send_ref, keep_ref, row_ref, bwd_ref, out_ref, grad_ref, ext, wide, narrow,
):
    sy = sy_ref[0]
    for y in range(NY):
        wide[pl.ds(y, CO, stride=NX * NY), :] = got_ref[2, y].astype(F32) + keep_ref[1, y].astype(F32)
        wide[pl.ds(NY + y, CO, stride=NX * NY), :] = keep_ref[2, y].astype(F32)
        ext[0, y + 1] = got_ref[0, y]
        ext[1, y + 1] = plus(got_ref[1, y], keep_ref[0, y])
        ext[2, y + 1] = send_ref[0, y]
        ext[3, y + 1] = send_ref[1, y]
    out_ref[...] = wide[...].reshape(CO, NX, NY, NZ).astype(BF)
    for x in range(4):
        ext[x, sy * (NY + 1)] = jnp.zeros(ext.shape[2:], BF)
        ext[x, (1 - sy) * (NY + 1)] = row_ref[x]
    for x in range(NX):
        for y in range(0, NY, 2):
            first, second = window(ext, x, y, CO)
            cols = jnp.concatenate([first, second], axis=1)
            part = jnp.dot(bwd_ref[...], cols, preferred_element_type=F32)
            for k in range(2):
                at = slice(k * NZ, (k + 1) * NZ)
                g = (
                    moved(part[:CI, at], -1)
                    + part[CI : 2 * CI, at]
                    + moved(part[2 * CI :, at], 1)
                )
                narrow[pl.ds(x * NY + y + k, CI, stride=NX * NY), :] = g
    grad_ref[...] = narrow[...].reshape(CI, NX, NY, NZ).astype(BF)


def finish(norm_ref, s_ref, w_ref, b_ref):
    norm = norm_ref[0]
    n, half = 9 * CI, 9 * CI // 2
    total = s_ref[...].astype(F32) * norm
    for ab in range(9):
        at = ab * CI
        w_ref[(ab * 3) * CI : (ab * 3 + 1) * CI, :] = total[at : at + CI, :CO]
        w_ref[(ab * 3 + 1) * CI : (ab * 3 + 2) * CI, :] = pltpu.roll(
            total[at : at + CI, :], CO, 1
        )[:, :CO]
    last = jnp.concatenate(
        [total[n : n + half], pltpu.roll(total[n : n + half], CO, 1)], axis=0
    )[:, :CO]
    for ab in range(9):
        w_ref[(ab * 3 + 2) * CI : (ab * 3 + 3) * CI, :] = last[ab * CI : (ab + 1) * CI]
    b_ref[...] = pltpu.roll(total[n + half : n + half + 8, :], CO, 1)[0:1, :CO]


def everywhere(blocks, axis):
    return lax.all_to_all(blocks, axis, 0, 0, tiled=True)


def copies(share, axis):
    return everywhere(jnp.broadcast_to(share[None], (lax.axis_size(axis), *share.shape)), axis)


def total(blocks):
    return jnp.sum(blocks.astype(F32), axis=0).astype(blocks.dtype)


def reduced(part):
    shares = lax.axis_size("plane")
    share = everywhere(part.reshape(shares, ROWS // shares, NZ), "plane")
    share = total(share)
    share = copies(share, GROUP)
    share = total(share)
    share = copies(share, "plane")
    return share.reshape(ROWS, NZ)


def per_device(volume, kernel, bias, upstream):
    s = pltpu.VMEM
    n = lax.axis_size("sx")
    up_line = [(i, i + 1) for i in range(n - 1)]
    down_line = [(j, i) for i, j in up_line]
    swap = [(0, 1), (1, 0)]
    sy = lax.axis_index("sy").astype(jnp.int32).reshape(1)
    sx = lax.axis_index("sx").astype(jnp.int32).reshape(1)
    here = (1 - lax.axis_index("sy")) * (NY - 1)
    taps = jnp.transpose(kernel, (2, 3, 4, 1, 0)).reshape(27 * CI, CO)
    own, row = call(
        turn_volume, (s((NX, NY, CI, NZ), BF), s((NX, CI, NZ), BF)),
        [pltpu.VMEM((CI * NX * NY, NZ), F32)], 2, 1, 10**8,
    )(sy, volume[0])
    after = lax.ppermute(own, "sx", down_line)
    fwd, bwd, lo, hi, bias_wide = call(
        prepare,
        (
            s((3 * CO, 9 * CI), BF), s((3 * CI, 9 * CO), BF), s((NY, CO, NZ), BF), s((NY, CO, NZ), BF),
            s((CO, NZ), F32),
        ),
        [pltpu.VMEM((CO * NX * NY, NZ), F32)], 3, 0, 10**9,
    )(taps, bias.reshape(1, CO), upstream[0])
    up = lax.ppermute(lo, "sx", down_line)
    edges = lax.dynamic_index_in_dim(after, here, 1, keepdims=False)
    swapped = lax.ppermute(jnp.concatenate([row, edges], axis=0), "sy", swap)
    parts = (s((3, NY, CO, NZ), BF), s((3, NY, CO, NZ), BF))
    sums = (9 * CI + 16, 2 * NZ)
    early = call(
        forward_near, (*parts, s(sums, F32)), [pltpu.VMEM((5, NY + 2, CI, NZ), BF)], 9, 2, 3 * 10**9,
    )(sy, sx, own, after, fwd, lo, hi, up, bias_wide)
    send, keep, edge, part = call(
        forward_far, (*parts, s((4, CO, NZ), BF), s((ROWS, NZ), BF)),
        [pltpu.VMEM((5, 4, CI, NZ), BF), pltpu.VMEM(sums, F32)], 13, 2, 10**9,
    )(sy, sx, own, after, swapped, fwd, lo, hi, up, bias_wide, *early)
    got = lax.ppermute(send, "sx", up_line)
    summed = reduced(part)
    edges = lax.dynamic_index_in_dim(got[:2], here, 1, keepdims=False)
    edges = edge + jnp.concatenate([edges, jnp.zeros_like(edges)], axis=0)
    swapped = lax.ppermute(edges, "sy", swap)
    o = jax.ShapeDtypeStruct
    out, grad = call(
        backward,
        (o((CO, NX, NY, NZ), BF), o((CI, NX, NY, NZ), BF)),
        [
            pltpu.VMEM((4, NY + 2, CO, NZ), BF),
            pltpu.VMEM((CO * NX * NY, NZ), F32),
            pltpu.VMEM((CI * NX * NY, NZ), F32),
        ],
        6, 1, 4 * 10**9,
    )(sy, got, send, keep, swapped, bwd)
    whole = lax.axis_size("plane") * lax.axis_size(GROUP) * NX * NY * NZ
    norm = (1.0 / jnp.sqrt(jnp.float32(whole))).reshape(1)
    w, b = call(finish, (o((27 * CI, CO), F32), o((1, CO), F32)), (), 2, 1, 10**8)(norm, summed)
    wgrad = jnp.transpose(w.reshape(3, 3, 3, CI, CO), (4, 3, 0, 1, 2))
    return out[None], grad[None], wgrad, b.reshape(CO)


def solution(mesh):
    cores = 2
    samp, sx, sy = mesh.devices.shape
    mesh = Mesh(mesh.devices.reshape(samp // cores, cores, sx, sy), ("plane", "core", "sx", "sy"))
    spec = P(SAMP, None, "sx", "sy", None)
    return jax.shard_map(
        per_device, mesh=mesh, in_specs=(spec, P(), P(), spec), out_specs=(spec, spec, P(), P()), check_vma=False
    )
```

```python
import jax
import jax.numpy as jnp
from jax import lax
from jax.experimental import pallas as pl
from jax.experimental.pallas import tpu as pltpu
from jax.sharding import Mesh
from jax.sharding import PartitionSpec as P


BF = jnp.bfloat16
F32 = jnp.float32
CI, CO, NX, NY, NZ = 32, 64, 2, 8, 128
GROUP = ("core", "sx", "sy")
SAMP = ("plane", "core")
NT_DIMS = (((1,), (1,)), ((), ()))
VM = pl.BlockSpec(memory_space=pltpu.VMEM)
SM = pl.BlockSpec(memory_space=pltpu.SMEM)
ROWS = 512


def call(body, outs, scratch=(), n_in=1, smem=0, flops=0):
    inner = pl.pallas_call(
        body,
        out_shape=outs,
        in_specs=[SM] * smem + [VM] * (n_in - smem),
        out_specs=jax.tree.map(lambda _: VM, outs),
        scratch_shapes=list(scratch),
        cost_estimate=pl.CostEstimate(flops=flops, bytes_accessed=1 << 20, transcendentals=0),
    )

    def run(*args):
        near = [pltpu.with_memory_space_constraint(a, pltpu.VMEM) for a in args[smem:]]
        return inner(*args[:smem], *near)

    return run


def turn_volume(sy_ref, v_ref, own_ref, edge_ref, buf):
    buf[...] = v_ref[...].astype(F32).reshape(CI * NX * NY, NZ)
    for x in range(NX):
        for y in range(NY):
            own_ref[x, y] = buf[pl.ds(x * NY + y, CI, stride=NX * NY), :].astype(BF)
    edge = (1 - sy_ref[0]) * (NY - 1)
    for x in range(NX):
        edge_ref[x] = own_ref[x, edge]


def prepare(w_ref, b_ref, u_ref, fwd_ref, bwd_ref, lo_ref, hi_ref, wide_ref, buf):
    eye = lax.broadcasted_iota(jnp.int32, (CO, CO), 0) == lax.broadcasted_iota(jnp.int32, (CO, CO), 1)
    column = jnp.sum(jnp.where(eye, b_ref[...], 0.0), axis=1, keepdims=True)
    wide_ref[...] = jnp.broadcast_to(column, (CO, NZ))
    eye = eye.astype(BF)
    for c in range(3):
        taps = jnp.concatenate(
            [w_ref[(ab * 3 + c) * CI : (ab * 3 + c + 1) * CI, :] for ab in range(9)], axis=0
        )
        fwd_ref[c * CO : (c + 1) * CO, :] = lax.dot_general(
            eye, taps, NT_DIMS, preferred_element_type=F32
        ).astype(BF)
        for ab in range(9):
            back = (2 - ab // 3) * 3 + 2 - ab % 3
            bwd_ref[c * CI : (c + 1) * CI, back * CO : (back + 1) * CO] = w_ref[
                (ab * 3 + c) * CI : (ab * 3 + c + 1) * CI, :
            ]
    buf[...] = u_ref[...].astype(F32).reshape(CO * NX * NY, NZ)
    for y in range(NY):
        lo_ref[y] = buf[pl.ds(y, CO, stride=NX * NY), :].astype(BF)
        hi_ref[y] = buf[pl.ds(NY + y, CO, stride=NX * NY), :].astype(BF)


def window(ext, x, y, channels):
    parts = []
    for dy in range(2):
        parts.append(
            jnp.concatenate(
                [ext[x + a, pl.ds(y + dy, 3)].reshape(3 * channels, NZ) for a in range(3)], axis=0
            )
        )
    return parts


def moved(v, shift):
    lane = lax.broadcasted_iota(jnp.int32, v.shape, 1)
    if shift == 1:
        return jnp.where(lane == 0, 0.0, pltpu.roll(v, 1, 1))
    return jnp.where(lane == NZ - 1, 0.0, pltpu.roll(v, NZ - 1, 1))


def two_rows(ext, x, y, at_y, first_x, fwd_ref, ups, bias_ref, acts, deltas):
    ones = jnp.ones((16, 2 * NZ), BF)
    none = jnp.zeros((CO, 2 * NZ), BF)
    first, second = window(ext, x, y, CI)
    cols = jnp.concatenate([first, second], axis=1)
    part = jnp.dot(fwd_ref[...], cols, preferred_element_type=F32)
    shifted = [[], [], []]
    for k in range(2):
        at = slice(k * NZ, (k + 1) * NZ)
        pre = (
            moved(part[:CO, at], 1)
            + part[CO : 2 * CO, at]
            + moved(part[2 * CO :, at], -1)
            + bias_ref[...]
        )
        e = jnp.exp(-jnp.abs(pre))
        r = 1.0 / (1.0 + e)
        sig = jnp.where(pre >= 0, r, e * r)
        soft = jnp.maximum(pre, 0.0) + jnp.log1p(e)
        act = 0.3 * pre + 0.7 * soft
        grad = ups[x][at_y + k].astype(F32) * (0.3 + 0.7 * sig)
        if x == 0:
            act = jnp.where(first_x, act, 0.0)
            grad = jnp.where(first_x, grad, 0.0)
        acts[x][at_y + k] = act.astype(BF)
        d = grad.astype(BF)
        deltas[x][at_y + k] = d
        wide = d.astype(F32)
        shifted[0].append(moved(wide, -1).astype(BF))
        shifted[1].append(d)
        shifted[2].append(moved(wide, 1).astype(BF))
    right = jnp.concatenate([jnp.concatenate(s, axis=1) for s in shifted] + [none], axis=0)
    left = jnp.concatenate([cols, ones], axis=0)
    return lax.dot_general(left, right, NT_DIMS, preferred_element_type=F32)


def places(send_ref, keep_ref, last_ref):
    acts = (keep_ref.at[1], keep_ref.at[2], last_ref)
    return acts, (keep_ref.at[0], send_ref.at[0], send_ref.at[1])


def forward_near(
    sy_ref, sx_ref, own_ref, next_ref, fwd_ref, lo_ref, hi_ref, up_ref, bias_ref,
    send_ref, keep_ref, last_ref, acc, ext,
):
    sy = sy_ref[0]
    ext[0] = jnp.zeros(ext.shape[1:], BF)
    for x, plane in enumerate((own_ref.at[0], own_ref.at[1], next_ref.at[0], next_ref.at[1])):
        for y in range(NY):
            ext[x + 1, y + 1] = plane[y]
        ext[x + 1, sy * (NY + 1)] = jnp.zeros(ext.shape[2:], BF)
        ext[x + 1, (1 - sy) * (NY + 1)] = jnp.zeros(ext.shape[2:], BF)
    acts, deltas = places(send_ref, keep_ref, last_ref)
    ups = (lo_ref, hi_ref, up_ref)
    far = (1 - sy) * (NY - 2)
    for x in range(NX + 1):
        for j in range(NY // 2 - 1):
            y = 2 * j + 2 * sy
            part = two_rows(ext, x, y, y, sx_ref[0] == 0, fwd_ref, ups, bias_ref, acts, deltas)
            if x + j:
                acc[...] += part
            else:
                acc[...] = part
        for k in range(2):
            acts[x][far + k] = jnp.zeros((CO, NZ), BF)
            deltas[x][far + k] = jnp.zeros((CO, NZ), BF)


def forward_far(
    sy_ref, sx_ref, own_ref, next_ref, row_ref, fwd_ref, lo_ref, hi_ref, up_ref, bias_ref, send_in, keep_in,
    last_in, acc_in, send_ref, keep_ref, last_ref, edge_ref, sum_ref, ext, acc,
):
    sy = sy_ref[0]
    send_ref[...] = send_in[...]
    keep_ref[...] = keep_in[...]
    last_ref[...] = last_in[...]
    ext[0] = jnp.zeros(ext.shape[1:], BF)
    for x, plane in enumerate((own_ref.at[0], own_ref.at[1], next_ref.at[0], next_ref.at[1])):
        for y in range(3):
            ext[x + 1, sy + y] = plane[(1 - sy) * (NY - 3) + y]
        ext[x + 1, 3 * (1 - sy)] = row_ref[x]
    acts, deltas = places(send_ref, keep_ref, last_ref)
    ups = (lo_ref, hi_ref, up_ref)
    far = (1 - sy) * (NY - 2)
    acc[...] = acc_in[...]
    for x in range(NX + 1):
        acc[...] += two_rows(ext, x, 0, far, sx_ref[0] == 0, fwd_ref, ups, bias_ref, acts, deltas)
    edge = (1 - sy) * (NY - 1)
    edge_ref[0] = jnp.zeros((CO, NZ), BF)
    for x in range(NX + 1):
        edge_ref[x + 1] = deltas[x][edge]
    n = 9 * CI
    sum_ref[0:n, :] = acc[0:n, 0:NZ].astype(sum_ref.dtype)
    half = n // 2
    sum_ref[n : n + half, :] = (
        acc[0:half, NZ:] + pltpu.roll(acc[half:n, NZ:], CO, 1)
    ).astype(sum_ref.dtype)
    sum_ref[n + half : n + half + 8, :] = acc[n : n + 8, 0:NZ].astype(sum_ref.dtype)
    sum_ref[n + half + 8 :, :] = jnp.zeros((ROWS - n - half - 8, NZ), sum_ref.dtype)


def plus(a, b):
    return (a.astype(F32) + b.astype(F32)).astype(BF)


def backward(
    sy_ref, got_ref, act_ref, send_ref, keep_ref, row_ref, bwd_ref, out_ref, grad_ref, ext, wide, narrow,
):
    sy = sy_ref[0]
    for y in range(NY):
        wide[pl.ds(y, CO, stride=NX * NY), :] = act_ref[y].astype(F32) + keep_ref[1, y].astype(F32)
        wide[pl.ds(NY + y, CO, stride=NX * NY), :] = keep_ref[2, y].astype(F32)
        ext[0, y + 1] = got_ref[0, y]
        ext[1, y + 1] = plus(got_ref[1, y], keep_ref[0, y])
        ext[2, y + 1] = send_ref[0, y]
        ext[3, y + 1] = send_ref[1, y]
    out_ref[...] = wide[...].reshape(CO, NX, NY, NZ).astype(BF)
    for x in range(4):
        ext[x, sy * (NY + 1)] = jnp.zeros(ext.shape[2:], BF)
        ext[x, (1 - sy) * (NY + 1)] = row_ref[x]
    for x in range(NX):
        for y in range(0, NY, 2):
            first, second = window(ext, x, y, CO)
            cols = jnp.concatenate([first, second], axis=1)
            part = jnp.dot(bwd_ref[...], cols, preferred_element_type=F32)
            for k in range(2):
                at = slice(k * NZ, (k + 1) * NZ)
                g = (
                    moved(part[:CI, at], -1)
                    + part[CI : 2 * CI, at]
                    + moved(part[2 * CI :, at], 1)
                )
                narrow[pl.ds(x * NY + y + k, CI, stride=NX * NY), :] = g
    grad_ref[...] = narrow[...].reshape(CI, NX, NY, NZ).astype(BF)


def finish(norm_ref, s_ref, w_ref, b_ref):
    norm = norm_ref[0]
    n, half = 9 * CI, 9 * CI // 2
    total = s_ref[...].astype(F32) * norm
    for ab in range(9):
        at = ab * CI
        w_ref[(ab * 3) * CI : (ab * 3 + 1) * CI, :] = total[at : at + CI, :CO]
        w_ref[(ab * 3 + 1) * CI : (ab * 3 + 2) * CI, :] = pltpu.roll(
            total[at : at + CI, :], CO, 1
        )[:, :CO]
    last = jnp.concatenate(
        [total[n : n + half], pltpu.roll(total[n : n + half], CO, 1)], axis=0
    )[:, :CO]
    for ab in range(9):
        w_ref[(ab * 3 + 2) * CI : (ab * 3 + 3) * CI, :] = last[ab * CI : (ab + 1) * CI]
    b_ref[...] = pltpu.roll(total[n + half : n + half + 8, :], CO, 1)[0:1, :CO]


def everywhere(blocks, axis):
    return lax.all_to_all(blocks, axis, 0, 0, tiled=True)


def copies(share, axis):
    return everywhere(jnp.broadcast_to(share[None], (lax.axis_size(axis), *share.shape)), axis)


def total(blocks):
    return jnp.sum(blocks.astype(F32), axis=0).astype(blocks.dtype)


def reduced(part):
    shares = lax.axis_size("plane")
    share = everywhere(part.reshape(shares, ROWS // shares, NZ), "plane")
    share = total(share)
    share = copies(share, GROUP)
    share = total(share)
    share = copies(share, "plane")
    return share.reshape(ROWS, NZ)


def per_device(volume, kernel, bias, upstream):
    s = pltpu.VMEM
    n = lax.axis_size("sx")
    up_line = [(i, i + 1) for i in range(n - 1)]
    down_line = [(j, i) for i, j in up_line]
    swap = [(0, 1), (1, 0)]
    sy = lax.axis_index("sy").astype(jnp.int32).reshape(1)
    sx = lax.axis_index("sx").astype(jnp.int32).reshape(1)
    here = (1 - lax.axis_index("sy")) * (NY - 1)
    taps = jnp.transpose(kernel, (2, 3, 4, 1, 0)).reshape(27 * CI, CO)
    own, row = call(
        turn_volume, (s((NX, NY, CI, NZ), BF), s((NX, CI, NZ), BF)),
        [pltpu.VMEM((CI * NX * NY, NZ), F32)], 2, 1, 10**8,
    )(sy, volume[0])
    after = lax.ppermute(own, "sx", down_line)
    fwd, bwd, lo, hi, bias_wide = call(
        prepare,
        (
            s((3 * CO, 9 * CI), BF), s((3 * CI, 9 * CO), BF), s((NY, CO, NZ), BF), s((NY, CO, NZ), BF),
            s((CO, NZ), F32),
        ),
        [pltpu.VMEM((CO * NX * NY, NZ), F32)], 3, 0, 10**9,
    )(taps, bias.reshape(1, CO), upstream[0])
    up = lax.ppermute(lo, "sx", down_line)
    edges = lax.dynamic_index_in_dim(after, here, 1, keepdims=False)
    swapped = lax.ppermute(jnp.concatenate([row, edges], axis=0), "sy", swap)
    parts = (s((2, NY, CO, NZ), BF), s((3, NY, CO, NZ), BF), s((NY, CO, NZ), BF))
    sums = (9 * CI + 16, 2 * NZ)
    early = call(
        forward_near, (*parts, s(sums, F32)), [pltpu.VMEM((5, NY + 2, CI, NZ), BF)], 9, 2, 3 * 10**9,
    )(sy, sx, own, after, fwd, lo, hi, up, bias_wide)
    send, keep, last, edge, part = call(
        forward_far, (*parts, s((4, CO, NZ), BF), s((ROWS, NZ), BF)),
        [pltpu.VMEM((5, 4, CI, NZ), BF), pltpu.VMEM(sums, F32)], 14, 2, 10**9,
    )(sy, sx, own, after, swapped, fwd, lo, hi, up, bias_wide, *early)
    got = lax.ppermute(send, "sx", up_line)
    summed = reduced(part)
    edges = lax.dynamic_index_in_dim(got, here, 1, keepdims=False)
    edges = edge + jnp.concatenate([edges, jnp.zeros_like(edges)], axis=0)
    swapped = lax.ppermute(edges, "sy", swap)
    act = lax.ppermute(last, "sx", up_line)
    o = jax.ShapeDtypeStruct
    out, grad = call(
        backward,
        (o((CO, NX, NY, NZ), BF), o((CI, NX, NY, NZ), BF)),
        [
            pltpu.VMEM((4, NY + 2, CO, NZ), BF),
            pltpu.VMEM((CO * NX * NY, NZ), F32),
            pltpu.VMEM((CI * NX * NY, NZ), F32),
        ],
        7, 1, 4 * 10**9,
    )(sy, got, act, send, keep, swapped, bwd)
    whole = lax.axis_size("plane") * lax.axis_size(GROUP) * NX * NY * NZ
    norm = (1.0 / jnp.sqrt(jnp.float32(whole))).reshape(1)
    w, b = call(finish, (o((27 * CI, CO), F32), o((1, CO), F32)), (), 2, 1, 10**8)(norm, summed)
    wgrad = jnp.transpose(w.reshape(3, 3, 3, CI, CO), (4, 3, 0, 1, 2))
    return out[None], grad[None], wgrad, b.reshape(CO)


def solution(mesh):
    cores = 2
    samp, sx, sy = mesh.devices.shape
    mesh = Mesh(mesh.devices.reshape(samp // cores, cores, sx, sy), ("plane", "core", "sx", "sy"))
    spec = P(SAMP, None, "sx", "sy", None)
    return jax.shard_map(
        per_device, mesh=mesh, in_specs=(spec, P(), P(), spec), out_specs=(spec, spec, P(), P()), check_vma=False
    )
```

```python
import jax
import jax.numpy as jnp
from jax import lax
from jax.experimental import pallas as pl
from jax.experimental.pallas import tpu as pltpu
from jax.sharding import Mesh
from jax.sharding import PartitionSpec as P


BF = jnp.bfloat16
F32 = jnp.float32
CI, CO, NX, NY, NZ = 32, 64, 2, 8, 128
GROUP = ("sx", "sy")
SAMP = ("plane", "core")
NT_DIMS = (((1,), (1,)), ((), ()))
VM = pl.BlockSpec(memory_space=pltpu.VMEM)
SM = pl.BlockSpec(memory_space=pltpu.SMEM)
ROWS = 512


def call(body, outs, scratch=(), n_in=1, smem=0, flops=0):
    inner = pl.pallas_call(
        body,
        out_shape=outs,
        in_specs=[SM] * smem + [VM] * (n_in - smem),
        out_specs=jax.tree.map(lambda _: VM, outs),
        scratch_shapes=list(scratch),
        cost_estimate=pl.CostEstimate(flops=flops, bytes_accessed=1 << 20, transcendentals=0),
    )

    def run(*args):
        near = [pltpu.with_memory_space_constraint(a, pltpu.VMEM) for a in args[smem:]]
        return inner(*args[:smem], *near)

    return run


def turn_volume(sy_ref, v_ref, own_ref, edge_ref, buf):
    buf[...] = v_ref[...].astype(F32).reshape(CI * NX * NY, NZ)
    for x in range(NX):
        for y in range(NY):
            own_ref[x, y] = buf[pl.ds(x * NY + y, CI, stride=NX * NY), :].astype(BF)
    edge = (1 - sy_ref[0]) * (NY - 1)
    for x in range(NX):
        edge_ref[x] = own_ref[x, edge]


def prepare(w_ref, b_ref, u_ref, fwd_ref, bwd_ref, lo_ref, hi_ref, wide_ref, buf):
    eye = lax.broadcasted_iota(jnp.int32, (CO, CO), 0) == lax.broadcasted_iota(jnp.int32, (CO, CO), 1)
    column = jnp.sum(jnp.where(eye, b_ref[...], 0.0), axis=1, keepdims=True)
    wide_ref[...] = jnp.broadcast_to(column, (CO, NZ))
    eye = eye.astype(BF)
    for c in range(3):
        taps = jnp.concatenate(
            [w_ref[(ab * 3 + c) * CI : (ab * 3 + c + 1) * CI, :] for ab in range(9)], axis=0
        )
        fwd_ref[c * CO : (c + 1) * CO, :] = lax.dot_general(
            eye, taps, NT_DIMS, preferred_element_type=F32
        ).astype(BF)
        for ab in range(9):
            back = (2 - ab // 3) * 3 + 2 - ab % 3
            bwd_ref[c * CI : (c + 1) * CI, back * CO : (back + 1) * CO] = w_ref[
                (ab * 3 + c) * CI : (ab * 3 + c + 1) * CI, :
            ]
    buf[...] = u_ref[...].astype(F32).reshape(CO * NX * NY, NZ)
    for y in range(NY):
        lo_ref[y] = buf[pl.ds(y, CO, stride=NX * NY), :].astype(BF)
        hi_ref[y] = buf[pl.ds(NY + y, CO, stride=NX * NY), :].astype(BF)


def window(ext, x, y, channels):
    parts = []
    for dy in range(2):
        parts.append(
            jnp.concatenate(
                [ext[x + a, pl.ds(y + dy, 3)].reshape(3 * channels, NZ) for a in range(3)], axis=0
            )
        )
    return parts


def moved(v, shift):
    lane = lax.broadcasted_iota(jnp.int32, v.shape, 1)
    if shift == 1:
        return jnp.where(lane == 0, 0.0, pltpu.roll(v, 1, 1))
    return jnp.where(lane == NZ - 1, 0.0, pltpu.roll(v, NZ - 1, 1))


def two_rows(ext, x, y, at_y, first_x, fwd_ref, ups, bias_ref, acts, deltas):
    ones = jnp.ones((16, 2 * NZ), BF)
    none = jnp.zeros((CO, 2 * NZ), BF)
    first, second = window(ext, x, y, CI)
    cols = jnp.concatenate([first, second], axis=1)
    part = jnp.dot(fwd_ref[...], cols, preferred_element_type=F32)
    shifted = [[], [], []]
    for k in range(2):
        at = slice(k * NZ, (k + 1) * NZ)
        pre = (
            moved(part[:CO, at], 1)
            + part[CO : 2 * CO, at]
            + moved(part[2 * CO :, at], -1)
            + bias_ref[...]
        )
        e = jnp.exp(-jnp.abs(pre))
        r = 1.0 / (1.0 + e)
        sig = jnp.where(pre >= 0, r, e * r)
        soft = jnp.maximum(pre, 0.0) + jnp.log1p(e)
        act = 0.3 * pre + 0.7 * soft
        grad = ups[x][at_y + k].astype(F32) * (0.3 + 0.7 * sig)
        if x == 0:
            act = jnp.where(first_x, act, 0.0)
            grad = jnp.where(first_x, grad, 0.0)
        acts[x][at_y + k] = act.astype(BF)
        d = grad.astype(BF)
        deltas[x][at_y + k] = d
        wide = d.astype(F32)
        shifted[0].append(moved(wide, -1).astype(BF))
        shifted[1].append(d)
        shifted[2].append(moved(wide, 1).astype(BF))
    right = jnp.concatenate([jnp.concatenate(s, axis=1) for s in shifted] + [none], axis=0)
    left = jnp.concatenate([cols, ones], axis=0)
    return lax.dot_general(left, right, NT_DIMS, preferred_element_type=F32)


def places(send_ref, keep_ref):
    acts = (keep_ref.at[1], keep_ref.at[2], send_ref.at[2])
    return acts, (keep_ref.at[0], send_ref.at[0], send_ref.at[1])


def forward_near(
    sy_ref, sx_ref, own_ref, next_ref, fwd_ref, lo_ref, hi_ref, up_ref, bias_ref,
    send_ref, keep_ref, acc, ext,
):
    sy = sy_ref[0]
    ext[0] = jnp.zeros(ext.shape[1:], BF)
    for x, plane in enumerate((own_ref.at[0], own_ref.at[1], next_ref.at[0], next_ref.at[1])):
        for y in range(NY):
            ext[x + 1, y + 1] = plane[y]
        ext[x + 1, sy * (NY + 1)] = jnp.zeros(ext.shape[2:], BF)
        ext[x + 1, (1 - sy) * (NY + 1)] = jnp.zeros(ext.shape[2:], BF)
    acts, deltas = places(send_ref, keep_ref)
    ups = (lo_ref, hi_ref, up_ref)
    far = (1 - sy) * (NY - 2)
    for x in range(NX + 1):
        for j in range(NY // 2 - 1):
            y = 2 * j + 2 * sy
            part = two_rows(ext, x, y, y, sx_ref[0] == 0, fwd_ref, ups, bias_ref, acts, deltas)
            if x + j:
                acc[...] += part
            else:
                acc[...] = part
        for k in range(2):
            acts[x][far + k] = jnp.zeros((CO, NZ), BF)
            deltas[x][far + k] = jnp.zeros((CO, NZ), BF)


def forward_far(
    sy_ref, sx_ref, own_ref, next_ref, row_ref, fwd_ref, lo_ref, hi_ref, up_ref, bias_ref, send_in, keep_in, acc_in,
    send_ref, keep_ref, edge_ref, sum_ref, ext, acc,
):
    sy = sy_ref[0]
    send_ref[...] = send_in[...]
    keep_ref[...] = keep_in[...]
    ext[0] = jnp.zeros(ext.shape[1:], BF)
    for x, plane in enumerate((own_ref.at[0], own_ref.at[1], next_ref.at[0], next_ref.at[1])):
        for y in range(3):
            ext[x + 1, sy + y] = plane[(1 - sy) * (NY - 3) + y]
        ext[x + 1, 3 * (1 - sy)] = row_ref[x]
    acts, deltas = places(send_ref, keep_ref)
    ups = (lo_ref, hi_ref, up_ref)
    far = (1 - sy) * (NY - 2)
    acc[...] = acc_in[...]
    for x in range(NX + 1):
        acc[...] += two_rows(ext, x, 0, far, sx_ref[0] == 0, fwd_ref, ups, bias_ref, acts, deltas)
    edge = (1 - sy) * (NY - 1)
    edge_ref[0] = jnp.zeros((CO, NZ), BF)
    for x in range(NX + 1):
        edge_ref[x + 1] = deltas[x][edge]
    n = 9 * CI
    sum_ref[0:n, :] = acc[0:n, 0:NZ].astype(sum_ref.dtype)
    half = n // 2
    sum_ref[n : n + half, :] = (
        acc[0:half, NZ:] + pltpu.roll(acc[half:n, NZ:], CO, 1)
    ).astype(sum_ref.dtype)
    sum_ref[n + half : n + half + 8, :] = acc[n : n + 8, 0:NZ].astype(sum_ref.dtype)
    sum_ref[n + half + 8 :, :] = jnp.zeros((ROWS - n - half - 8, NZ), sum_ref.dtype)


def plus(a, b):
    return (a.astype(F32) + b.astype(F32)).astype(BF)


def backward(
    sy_ref, got_ref, send_ref, keep_ref, row_ref, bwd_ref, out_ref, grad_ref, ext, wide, narrow,
):
    sy = sy_ref[0]
    for y in range(NY):
        wide[pl.ds(y, CO, stride=NX * NY), :] = got_ref[2, y].astype(F32) + keep_ref[1, y].astype(F32)
        wide[pl.ds(NY + y, CO, stride=NX * NY), :] = keep_ref[2, y].astype(F32)
        ext[0, y + 1] = got_ref[0, y]
        ext[1, y + 1] = plus(got_ref[1, y], keep_ref[0, y])
        ext[2, y + 1] = send_ref[0, y]
        ext[3, y + 1] = send_ref[1, y]
    out_ref[...] = wide[...].reshape(CO, NX, NY, NZ).astype(BF)
    for x in range(4):
        ext[x, sy * (NY + 1)] = jnp.zeros(ext.shape[2:], BF)
        ext[x, (1 - sy) * (NY + 1)] = row_ref[x]
    for x in range(NX):
        for y in range(0, NY, 2):
            first, second = window(ext, x, y, CO)
            cols = jnp.concatenate([first, second], axis=1)
            part = jnp.dot(bwd_ref[...], cols, preferred_element_type=F32)
            for k in range(2):
                at = slice(k * NZ, (k + 1) * NZ)
                g = (
                    moved(part[:CI, at], -1)
                    + part[CI : 2 * CI, at]
                    + moved(part[2 * CI :, at], 1)
                )
                narrow[pl.ds(x * NY + y + k, CI, stride=NX * NY), :] = g
    grad_ref[...] = narrow[...].reshape(CI, NX, NY, NZ).astype(BF)


def finish(norm_ref, s_ref, w_ref, b_ref):
    norm = norm_ref[0]
    n, half = 9 * CI, 9 * CI // 2
    total = s_ref[...].astype(F32) * norm
    for ab in range(9):
        at = ab * CI
        w_ref[(ab * 3) * CI : (ab * 3 + 1) * CI, :] = total[at : at + CI, :CO]
        w_ref[(ab * 3 + 1) * CI : (ab * 3 + 2) * CI, :] = pltpu.roll(
            total[at : at + CI, :], CO, 1
        )[:, :CO]
    last = jnp.concatenate(
        [total[n : n + half], pltpu.roll(total[n : n + half], CO, 1)], axis=0
    )[:, :CO]
    for ab in range(9):
        w_ref[(ab * 3 + 2) * CI : (ab * 3 + 3) * CI, :] = last[ab * CI : (ab + 1) * CI]
    b_ref[...] = pltpu.roll(total[n + half : n + half + 8, :], CO, 1)[0:1, :CO]


def everywhere(blocks, axis):
    return lax.all_to_all(blocks, axis, 0, 0, tiled=True)


def copies(share, axis):
    return everywhere(jnp.broadcast_to(share[None], (lax.axis_size(axis), *share.shape)), axis)


def total(blocks):
    return jnp.sum(blocks.astype(F32), axis=0).astype(blocks.dtype)


def reduced(part):
    shares = lax.axis_size(SAMP)
    share = everywhere(part.reshape(shares, ROWS // shares, NZ), SAMP)
    share = total(share)
    share = copies(share, GROUP)
    share = total(share)
    share = copies(share, SAMP)
    return share.reshape(ROWS, NZ)


def per_device(volume, kernel, bias, upstream):
    s = pltpu.VMEM
    n = lax.axis_size("sx")
    up_line = [(i, i + 1) for i in range(n - 1)]
    down_line = [(j, i) for i, j in up_line]
    swap = [(0, 1), (1, 0)]
    sy = lax.axis_index("sy").astype(jnp.int32).reshape(1)
    sx = lax.axis_index("sx").astype(jnp.int32).reshape(1)
    here = (1 - lax.axis_index("sy")) * (NY - 1)
    taps = jnp.transpose(kernel, (2, 3, 4, 1, 0)).reshape(27 * CI, CO)
    own, row = call(
        turn_volume, (s((NX, NY, CI, NZ), BF), s((NX, CI, NZ), BF)),
        [pltpu.VMEM((CI * NX * NY, NZ), F32)], 2, 1, 10**8,
    )(sy, volume[0])
    after = lax.ppermute(own, "sx", down_line)
    fwd, bwd, lo, hi, bias_wide = call(
        prepare,
        (
            s((3 * CO, 9 * CI), BF), s((3 * CI, 9 * CO), BF), s((NY, CO, NZ), BF), s((NY, CO, NZ), BF),
            s((CO, NZ), F32),
        ),
        [pltpu.VMEM((CO * NX * NY, NZ), F32)], 3, 0, 10**9,
    )(taps, bias.reshape(1, CO), upstream[0])
    up = lax.ppermute(lo, "sx", down_line)
    edges = lax.dynamic_index_in_dim(after, here, 1, keepdims=False)
    swapped = lax.ppermute(jnp.concatenate([row, edges], axis=0), "sy", swap)
    parts = (s((3, NY, CO, NZ), BF), s((3, NY, CO, NZ), BF))
    sums = (9 * CI + 16, 2 * NZ)
    early = call(
        forward_near, (*parts, s(sums, F32)), [pltpu.VMEM((5, NY + 2, CI, NZ), BF)], 9, 2, 3 * 10**9,
    )(sy, sx, own, after, fwd, lo, hi, up, bias_wide)
    send, keep, edge, part = call(
        forward_far, (*parts, s((4, CO, NZ), BF), s((ROWS, NZ), BF)),
        [pltpu.VMEM((5, 4, CI, NZ), BF), pltpu.VMEM(sums, F32)], 13, 2, 10**9,
    )(sy, sx, own, after, swapped, fwd, lo, hi, up, bias_wide, *early)
    got = lax.ppermute(send, "sx", up_line)
    summed = reduced(part)
    edges = lax.dynamic_index_in_dim(got[:2], here, 1, keepdims=False)
    edges = edge + jnp.concatenate([edges, jnp.zeros_like(edges)], axis=0)
    swapped = lax.ppermute(edges, "sy", swap)
    o = jax.ShapeDtypeStruct
    out, grad = call(
        backward,
        (o((CO, NX, NY, NZ), BF), o((CI, NX, NY, NZ), BF)),
        [
            pltpu.VMEM((4, NY + 2, CO, NZ), BF),
            pltpu.VMEM((CO * NX * NY, NZ), F32),
            pltpu.VMEM((CI * NX * NY, NZ), F32),
        ],
        6, 1, 4 * 10**9,
    )(sy, got, send, keep, swapped, bwd)
    whole = lax.axis_size(SAMP) * lax.axis_size(GROUP) * NX * NY * NZ
    norm = (1.0 / jnp.sqrt(jnp.float32(whole))).reshape(1)
    w, b = call(finish, (o((27 * CI, CO), F32), o((1, CO), F32)), (), 2, 1, 10**8)(norm, summed)
    wgrad = jnp.transpose(w.reshape(3, 3, 3, CI, CO), (4, 3, 0, 1, 2))
    return out[None], grad[None], wgrad, b.reshape(CO)


def solution(mesh):
    cores = 2
    samp, sx, sy = mesh.devices.shape
    mesh = Mesh(mesh.devices.reshape(samp // cores, cores, sx, sy), ("plane", "core", "sx", "sy"))
    spec = P(SAMP, None, "sx", "sy", None)
    return jax.shard_map(
        per_device, mesh=mesh, in_specs=(spec, P(), P(), spec), out_specs=(spec, spec, P(), P()), check_vma=False
    )
```
